32 devices in a mesh: freq: 4 (over y, core), lat: 8 (over z, x).
Axes of the slice: x: 2, y: 2, z: 4, core: 2. Of those that a mesh axis runs over, the one named last changes fastest.
Arguments:
- spectra: float32 [2, 4, 32768], P(None, None, ('freq', 'lat')), may hold values from -6 to 6
- tile_route: int32 [32768, 1], P(('freq', 'lat')), may hold values from 0 to 255; in each aligned block of 1024 rows (0 to 1023, 1024 to 2047, ...) at most 8 rows name the same one
- bin_in_tile: int32 [32768], P(('freq', 'lat')), may hold values from 0 to 1023
- trace_offset: float32 [2, 32768], P(None, ('freq', 'lat')), may hold values from -0.5 to 0.5
- weights: float32 [32768], P(('freq', 'lat')), may hold values from 0.2 to 5
- frequency: float32 [4], P('freq'), may hold values from 0.5 to 1.5
- slowness: float32 [2, 8], replicated, may hold values from 0.6 to 1.6
- vel_index: int32 [2, 512, 512], P(None, 'lat'), may hold values from 0 to 7
Outputs:
- wavefield: float32 [2, 4, 512, 512], P(None, 'freq', 'lat')
- depth_image: float32 [2, 512, 512], P(None, 'lat', 'freq')
The draws below stay inside these ranges and needn't reach their ends.
Inputs may be any that keep to these rules, and one draw needn't show every extreme that they name: `tile_route`: tiles of 32 x 32 bins, numbered row by row over the grid; among the rows of one device no tile is named by more than 8 traces. `bin_in_tile`: row * 32 + column of the bin within the tile.
All inputs are finite; a program needn't handle non-finite values.
Results may differ from the reference program's by a relative error of at most 0.0003.
Values sent between devices are 32-bit elements; how exact they have to be, the bound alone decides.
A program may use at most 64 MiB of HBM per device.

```python
import math
import jax
import jax.numpy as jnp
import numpy as np
from jax import lax

NX = 512
NY = 512
TB = 32
MODES = 8
TR_DEV = 1024
NSTEPS = 2
NREF = 2
NVEL = 8
NF = 4
TRACES = 32768
TILES = 256
CAP = 8
N_LAT = 8
DEVICES = 32


def plant(values, rng, least, largest):
    shape = values.shape
    place = [jax.random.randint(jax.random.fold_in(rng, axis), (), 0, shape[axis]) for axis in range(len(shape))]
    values = values.at[tuple(place)].set(least)
    longest = shape.index(max(shape))
    place[longest] = (place[longest] + 1) % shape[longest]
    return values.at[tuple(place)].set(largest)


def block_scale(key, dims, shards, low, top_value):
    loudness, own = 1.0, jax.random.fold_in(key, 6)
    for dim, parts in shards:
        steps = jnp.exp(jax.random.uniform(jax.random.fold_in(own, dim), (parts,), jnp.float32, low / len(shards), top_value / len(shards)))
        loudness = loudness * jnp.repeat(steps, dims[dim] // parts).reshape([-1 if axis == dim else 1 for axis in range(len(dims))])
    return loudness


def shared_out(rng, own, number, rows, count, top, most, skew):
    order = jax.random.permutation(rng, count)
    heavy_load, common = load_shares(count, rows * top, most, skew, True), load_shares(count, rows * top, most, skew, False)
    places = jnp.arange(count)

    def named(sizes, turn):
        used = int((sizes > 0).sum())
        fixed = max(1, used // 4)
        moved = fixed + (places - fixed + turn * (used - fixed)) % max(1, count - fixed)
        return jnp.zeros((count,), jnp.int32).at[order[jnp.where(places < fixed, places, moved)]].set(jnp.asarray(sizes, jnp.int32))

    sizes = jnp.where(number % 4 == 0, named(heavy_load, number // 4), named(common, number - number // 4 - 1))
    mixed = jax.random.permutation(jax.random.fold_in(own, 3), count)
    donor, sink = mixed[0:count // 2 * 2:2], mixed[1:count // 2 * 2:2]
    room = jnp.minimum(sizes[donor] - 1, most - sizes[sink]) // 2
    room = jnp.where((donor == order[0]) | (sink == order[0]) | (sizes[sink] == 0), 0, jnp.maximum(room, 0))
    moved = jax.random.randint(jax.random.fold_in(own, 4), (count // 2,), 0, 1 << 20) % (room + 1)
    sizes = sizes.at[donor].add(-moved).at[sink].add(moved)
    labels = jnp.searchsorted(jnp.cumsum(sizes), jnp.arange(rows * top), side="right").astype(jnp.int32)
    table = labels.reshape(top, rows).T
    table = table[jax.random.permutation(jax.random.fold_in(own, 1), rows)]
    turn = jax.random.randint(jax.random.fold_in(own, 2), (rows, 1), 0, top)
    return jnp.take_along_axis(table, (jnp.arange(top)[None, :] + turn) % top, axis=1)


def load_shares(amount, total, reach, lean, full):
    portions = [(1 << 20) // math.isqrt(grade ** lean) + 1 for grade in range(1, amount + 1)]
    largest = reach if full else min(reach, max(-(-total // amount), total * portions[0] // sum(portions)))
    least = 1 if total - largest >= amount - 1 else 0
    given, spare = [largest] + [least] * (amount - 1), total - largest - least * (amount - 1)
    while spare > 0:
        candidates = [i for i in range(1, amount) if given[i] < largest] or [i for i in range(1, amount) if given[i] < reach]
        mass, budget = sum([portions[i] for i in candidates]), spare
        for i in candidates:
            more = min(reach - given[i], max(1, budget * portions[i] // mass), spare)
            given[i] = given[i] + more
            spare = spare - more
    return np.array(given)


def gaussian(key, dims, deviation, reach, pieces=(), kind=jnp.bfloat16):
    result = jax.random.normal(key, dims, jnp.float32) * deviation
    if len(pieces) > 0:
        result = block_scale(key, dims, pieces, -0.22, 0.18) * result
    return jnp.clip(result, min=-reach, max=reach).astype(kind)


def setup_inputs(seed: int = 0) -> dict:
    streams_of = jax.random.split(jax.random.key(seed), 9)
    spectra = gaussian(streams_of[0], (2, NF, TRACES), 1.0, 6.0, ((2, 32),), jnp.float32)
    tile_route_keys = jax.random.split(jax.random.fold_in(streams_of[1], 1), TRACES // TR_DEV)
    tile_route_turns = jax.random.permutation(jax.random.fold_in(streams_of[1], 3), TRACES // TR_DEV)
    tile_route = jax.vmap(lambda own, number: shared_out(jax.random.fold_in(streams_of[1], 2), own, number, TR_DEV, TILES, 1, CAP, 2))(tile_route_keys, tile_route_turns).reshape((TRACES, 1))
    bin_in_tile = plant(jax.random.randint(streams_of[2], (TRACES,), 0, TB * TB), jax.random.fold_in(streams_of[2], 1), 0, (TB * TB) - 1).astype(jnp.int32)
    trace_offset = jnp.clip(jax.random.uniform(streams_of[3], (2, TRACES), jnp.float32, -0.5, 0.5) * block_scale(streams_of[3], (2, TRACES), ((1, 32),), -0.4, 0.0), -0.5, 0.5)
    weights = jnp.clip(jnp.exp(math.log(5.0) - 3.218876 * jax.random.uniform(streams_of[4], (TRACES,), jnp.float32) ** block_scale(streams_of[4], (TRACES,), ((0, 32),), -0.2, 0.2)), 0.2, 5.0)
    frequency = jnp.clip(0.5 + 1.0 * jax.random.uniform(streams_of[5], (NF,), jnp.float32) ** block_scale(streams_of[5], (NF,), ((0, 4),), -0.2, 0.2), 0.5, 1.5)
    slowness = jnp.clip(jnp.exp(jax.random.uniform(streams_of[6], (NSTEPS, NVEL), jnp.float32, math.log(0.6), math.log(1.6))), 0.6, 1.6)
    vel_index = plant(jax.random.randint(streams_of[7], (NSTEPS, NX, NY), 0, NVEL), jax.random.fold_in(streams_of[7], 1), 0, NVEL - 1).astype(jnp.int32)
    return dict(spectra=spectra, tile_route=tile_route, bin_in_tile=bin_in_tile, trace_offset=trace_offset, weights=weights, frequency=frequency, slowness=slowness, vel_index=vel_index)


damping = 1.0
depth_step = 1.0

def basis_of(cell_x, cell_y):
    mode_ids = jnp.arange(MODES).astype(jnp.float32)
    along_x = jnp.cos(math.pi * mode_ids.reshape((MODES,) + (1,) * cell_x.ndim) * (cell_x[None] + 0.5) / TB)
    along_y = jnp.cos(math.pi * mode_ids.reshape((MODES,) + (1,) * cell_y.ndim) * (cell_y[None] + 0.5) / TB)
    return (along_x[:, None] * along_y[None, :]).reshape((MODES * MODES,) + cell_x.shape)

def fit_grid(normal, right_side, row_count):
    tile_count = normal.shape[0]
    system = normal + damping * jnp.eye(MODES * MODES, dtype=jnp.float32)
    factor = jnp.linalg.cholesky(system)
    flat_rhs = right_side.reshape(tile_count, MODES * MODES, -1)
    middle = jax.scipy.linalg.solve_triangular(factor, flat_rhs, lower=True)
    coeffs = jax.scipy.linalg.solve_triangular(factor, middle, lower=True, trans='T')
    coeffs = coeffs.reshape(row_count // TB, NY // TB, MODES, MODES, 2, -1)
    cell_pos = jnp.arange(TB).astype(jnp.float32)
    cos_table = jnp.cos(math.pi * jnp.arange(MODES).astype(jnp.float32)[:, None] * (cell_pos[None, :] + 0.5) / TB)
    viewed = jnp.einsum('xyabpq,ai,bj->pqxiyj', coeffs, cos_table, cos_table, precision=lax.Precision.HIGHEST)
    return viewed.reshape(2, viewed.shape[1], row_count, NY)

def reference(spectra, tile_route, bin_in_tile, trace_offset, weights, frequency, slowness, vel_index):
    tile_id = tile_route[:, 0].astype(jnp.int32)
    trace_count = tile_id.shape[0]
    per_tile = DEVICES * CAP
    ranking = jnp.argsort(tile_id, stable=True).astype(jnp.int32)
    sorted_tiles = tile_id[ranking]
    firsts = jnp.searchsorted(sorted_tiles, sorted_tiles, side='left').astype(jnp.int32)
    position = sorted_tiles * per_tile + jnp.arange(trace_count, dtype=jnp.int32) - firsts
    lookup = jnp.full((TILES * per_tile,), trace_count, jnp.int32).at[position].set(ranking)
    cell_x = (bin_in_tile // TB).astype(jnp.float32) + trace_offset[0]
    cell_y = (bin_in_tile % TB).astype(jnp.float32) + trace_offset[1]
    trace_meta = jnp.stack([weights, cell_x, cell_y], 0)
    padded_meta = jnp.concatenate([trace_meta, jnp.zeros((3, 1), jnp.float32)], 1)
    padded_spec = jnp.concatenate([spectra, jnp.zeros((2, NF, 1), jnp.float32)], 2)
    tile_dev = TILES // N_LAT
    row_count = NX // N_LAT

    def one_owner(owner_at):
        picks = lax.dynamic_slice_in_dim(lookup, owner_at * tile_dev * per_tile, tile_dev * per_tile)
        meta_here = padded_meta[:, picks].reshape(3, tile_dev, per_tile)
        spec_here = padded_spec[:, :, picks].reshape(2, NF, tile_dev, per_tile)
        basis_vals = basis_of(meta_here[1], meta_here[2])
        weighted = basis_vals * meta_here[0][None]
        normal = jnp.einsum('itc,jtc->tij', weighted, basis_vals, precision=lax.Precision.HIGHEST)
        right_side = jnp.einsum('itc,pqtc->tipq', weighted, spec_here, precision=lax.Precision.HIGHEST)
        return fit_grid(normal, right_side, row_count)
    slabs = lax.map(one_owner, jnp.arange(N_LAT, dtype=jnp.int32))
    gridded = jnp.moveaxis(slabs, 0, 2).reshape(2, NF, NX, NY)
    wave_field = gridded[0] + 1j * gridded[1]
    index_x = jnp.arange(NX)
    index_y = jnp.arange(NY)
    signed_x = jnp.where(index_x >= NX // 2, index_x - NX, index_x)
    signed_y = jnp.where(index_y >= NY // 2, index_y - NY, index_y)
    kx_vals = 2.0 * math.pi / NX * signed_x.astype(jnp.float32)
    ky_vals = 2.0 * math.pi / NY * signed_y.astype(jnp.float32)
    per_group = NVEL // NREF
    images = []
    for depth_at in range(NSTEPS):
        table_row = slowness[depth_at]
        references = table_row.reshape(NREF, per_group).mean(axis=1)
        spectrum = jnp.fft.fft2(wave_field)
        wave_num = frequency[None, :] * references[:, None]
        vertical = (wave_num * wave_num)[:, :, None, None] - (kx_vals * kx_vals)[None, None, :, None] - (ky_vals * ky_vals)[None, None, None, :]
        phase_angle = jnp.sqrt(jnp.maximum(vertical, 0.0)) * depth_step
        damped = jnp.exp(-jnp.sqrt(jnp.maximum(-vertical, 0.0)) * depth_step)
        returned = jnp.fft.ifft2(spectrum[None] * (damped * jnp.exp(1j * phase_angle)))
        velocity = vel_index[depth_at]
        local_slow = table_row[velocity]
        group_of = velocity // per_group
        split_phase = frequency[None, :, None, None] * (local_slow[None, None] - references[:, None, None, None]) * depth_step
        group_mask = group_of[None] == jnp.arange(NREF)[:, None, None]
        wave_field = lax.optimization_barrier(jnp.sum(jnp.where(group_mask[:, None], returned * jnp.exp(1j * split_phase), 0.0), 0))
        images.append(lax.optimization_barrier(jnp.sum(jnp.real(wave_field), 0)).astype(jnp.float32))
    wavefield = jnp.stack([jnp.real(wave_field), jnp.imag(wave_field)], 0).astype(jnp.float32)
    return (wavefield, jnp.stack(images, 0))
```

```python
import functools
import math

import jax
import jax.numpy as jnp
import numpy as np
from jax import lax
from jax.experimental import pallas as pl
from jax.experimental.pallas import tpu as pltpu
from jax.sharding import PartitionSpec as P

TB = 32
MODES = 8
CAP = 8
TERMS = MODES * MODES

damping = 1.0
depth_step = 1.0

NN = (((1,), (0,)), ((), ()))
NT = (((1,), (1,)), ((), ()))
VMEM = pl.BlockSpec(memory_space=pltpu.VMEM)


def dft_tables(length):
    at = np.arange(length)
    angle = 2.0 * math.pi / length * (at[:, None] * at[None, :] % length)
    exact = np.stack([np.cos(angle), np.sin(angle)], 0)
    high = exact.astype(jnp.bfloat16)
    low = (exact - high.astype(np.float64)).astype(jnp.bfloat16)
    return high, low


def mode_tables(length):
    at = np.arange(length)
    angle = 2.0 * math.pi / length * (at[:, None] * at[None, :] % length)
    cosines = np.cos(math.pi * np.arange(MODES)[:, None] * (np.arange(TB)[None, :] + 0.5) / TB)
    fold = np.zeros((length // TB, MODES, length))
    for tile in range(length // TB):
        fold[tile, :, tile * TB : (tile + 1) * TB] = cosines
    fold = fold.reshape(length // TB * MODES, length)
    return np.concatenate([fold @ np.cos(angle), -(fold @ np.sin(angle))], 1).astype(np.float32)


def split2(x):
    high = x.astype(jnp.bfloat16)
    return high, (x - high.astype(jnp.float32)).astype(jnp.bfloat16)


def dot3(a, b, dims=NN):
    one = functools.partial(lax.dot_general, dimension_numbers=dims, preferred_element_type=jnp.float32)
    return one(a[0], b[0]) + (one(a[0], b[1]) + one(a[1], b[0]))


def route_kernel(slot_ref, feat_ref, out_ref):
    feats = feat_ref[...]
    high = feats.astype(jnp.bfloat16)
    rest = feats - high.astype(jnp.float32)
    middle = rest.astype(jnp.bfloat16)
    low = (rest - middle.astype(jnp.float32)).astype(jnp.bfloat16)
    parts = jnp.concatenate([high, middle, low], 0)
    rows = feats.shape[0]
    slot = slot_ref[...]
    width = 256
    for at in range(0, out_ref.shape[1], width):
        places = lax.broadcasted_iota(jnp.int32, (width, slot.shape[1]), 0) + at
        chosen = jnp.where(places == slot, 1.0, 0.0).astype(jnp.bfloat16)
        got = lax.dot_general(parts, chosen, NT, preferred_element_type=jnp.float32)
        out_ref[:, at : at + width] = got[:rows] + got[rows : 2 * rows] + got[2 * rows :]


def fit_kernel(tiles, got_ref, out_ref, system):
    count = got_ref.shape[1]
    data_rows = got_ref.shape[0] - 3
    weight = got_ref[data_rows : data_rows + 1, :]

    def chebyshev(cosine):
        terms = [jnp.ones_like(cosine), cosine]
        for _ in range(MODES - 2):
            terms.append(2.0 * cosine * terms[-1] - terms[-2])
        return terms

    along_x = chebyshev(got_ref[data_rows + 1 : data_rows + 2, :])
    along_y = jnp.concatenate(chebyshev(got_ref[data_rows + 2 : data_rows + 3, :]), 0)
    basis = jnp.concatenate([term * along_y for term in along_x], 0)
    right = jnp.concatenate([basis, got_ref[:data_rows, :]], 0)
    weighted = basis * weight
    lane = lax.broadcasted_iota(jnp.int32, (1, count), 1)
    tile_of = lax.div(lax.rem(lane, tiles * CAP), CAP)
    width = TERMS + data_rows
    eye = jnp.where(
        lax.broadcasted_iota(jnp.int32, (TERMS, width), 0)
        == lax.broadcasted_iota(jnp.int32, (TERMS, width), 1),
        damping,
        0.0,
    )
    left = jnp.concatenate([jnp.where(tile_of == tile, weighted, 0.0) for tile in range(tiles)], 0)
    summed = lax.dot_general(
        left, right, NT, preferred_element_type=jnp.float32, precision=lax.Precision.HIGHEST
    )
    system[...] = summed.reshape(tiles, TERMS, width) + eye[None]
    for k in range(TERMS):
        row = system[:, k : k + 1, :]
        scaled = row * (1.0 / row[:, :, k : k + 1])
        whole = system[...]
        system[...] = whole - whole[:, :, k : k + 1] * scaled
        system[:, k : k + 1, :] = scaled
    out_ref[...] = system[:, :, TERMS:]


def bands(real, imag, out_ref):
    count = out_ref.shape[0]
    band = real.shape[1] // count
    for dst in range(count):
        part = slice(dst * band, (dst + 1) * band)
        out_ref[dst] = jnp.concatenate([real[:, part], imag[:, part]], 1)


def modes_y_kernel(coef_ref, table_ref, out_ref):
    rows = coef_ref.shape[0] // 2
    length = table_ref.shape[1] // 2
    made = lax.dot_general(
        coef_ref[...],
        table_ref[...],
        NN,
        preferred_element_type=jnp.float32,
        precision=lax.Precision.HIGHEST,
    )
    real = made[:rows, :length] - made[rows:, length:]
    imag = made[:rows, length:] + made[rows:, :length]
    bands(real, imag, out_ref)


def swapped(x):
    half = x.shape[1] // 2
    return jnp.concatenate([x[:, half:], x[:, :half]], 1)


def column_kernel(from_modes, high_ref, low_ref, table_ref, got_ref, even_ref, odd_ref, out_ref):
    lanes = got_ref.shape[2]
    got = got_ref[...].reshape(-1, lanes)
    sign = jnp.where(lax.broadcasted_iota(jnp.int32, (1, lanes), 1) < lanes // 2, -1.0, 1.0)
    cosine = (high_ref[0], low_ref[0])
    sine = (high_ref[1], low_ref[1])
    if from_modes:
        length = table_ref.shape[0] // 2
        both = lax.dot_general(
            table_ref[...],
            got,
            NN,
            preferred_element_type=jnp.float32,
            precision=lax.Precision.HIGHEST,
        )
        spectrum = both[:length] + sign * swapped(both[length:])
    else:
        parts = split2(got)
        spectrum = dot3(cosine, parts) - sign * swapped(dot3(sine, parts))
    turned = swapped(spectrum)
    refs = even_ref.shape[0]
    moved = jnp.concatenate(
        [spectrum * even_ref[g] + turned * odd_ref[g] for g in range(refs)], 1
    )
    parts = split2(moved)
    straight = dot3(cosine, parts)
    crossed = dot3(sine, parts)
    rows = out_ref.shape[2]
    for g in range(refs):
        part = slice(g * lanes, (g + 1) * lanes)
        back = straight[:, part] + sign * swapped(crossed[:, part])
        for dst in range(out_ref.shape[0]):
            out_ref[dst, g] = back[dst * rows : (dst + 1) * rows]


def row_kernel(last, high_ref, low_ref, got_ref, cos_ref, sin_ref, group_ref, *out_refs):
    wave_ref = out_refs[0]
    count, refs, rows, lanes = got_ref.shape
    half = lanes // 2
    cosine = (high_ref[0], low_ref[0])
    sine = (high_ref[1], low_ref[1])
    real = jnp.concatenate(
        [got_ref[src, :, :, :half].reshape(refs * rows, half) for src in range(count)], 1
    )
    imag = jnp.concatenate(
        [got_ref[src, :, :, half:].reshape(refs * rows, half) for src in range(count)], 1
    )
    parts = split2(jnp.concatenate([real, imag], 0))
    straight = dot3(parts, cosine)
    crossed = dot3(parts, sine)
    total = refs * rows
    real = straight[:total] - crossed[total:]
    imag = straight[total:] + crossed[:total]
    group = group_ref[...]
    chosen_real, chosen_imag = real[:rows], imag[:rows]
    for g in range(1, refs):
        part = slice(g * rows, (g + 1) * rows)
        chosen_real = jnp.where(group == g, real[part], chosen_real)
        chosen_imag = jnp.where(group == g, imag[part], chosen_imag)
    along, across = cos_ref[...], sin_ref[...]
    real = chosen_real * along - chosen_imag * across
    imag = chosen_real * across + chosen_imag * along
    wave_ref[0] = real
    if last:
        wave_ref[1] = imag
        return
    parts = split2(jnp.concatenate([real, imag], 0))
    straight = dot3(parts, cosine)
    crossed = dot3(parts, sine)
    bands(
        straight[:rows] + crossed[rows:],
        straight[rows:] - crossed[:rows],
        out_refs[1],
    )


def call(kernel, shapes, flops, *operands, scratch=()):
    single = not isinstance(shapes, (list, tuple))
    out_shape = jax.tree.map(
        lambda s: jax.ShapeDtypeStruct(s.shape, jnp.float32), shapes
    )
    return pl.pallas_call(
        kernel,
        out_shape=out_shape,
        in_specs=[VMEM] * len(operands),
        out_specs=VMEM if single else [VMEM] * len(shapes),
        scratch_shapes=list(scratch),
        cost_estimate=pl.CostEstimate(flops=flops, bytes_accessed=4 << 20, transcendentals=0),
        compiler_params=pltpu.CompilerParams(vmem_limit_bytes=48 << 20),
    )(*operands)


def shaped(*dims):
    return jax.ShapeDtypeStruct(dims, jnp.float32)


def local(spectra, tile_route, bin_in_tile, trace_offset, weights, frequency, slowness, vel_index):
    freq_count = lax.axis_size("freq")
    lat_count = lax.axis_size("lat")
    devices = freq_count * lat_count
    steps, row_count, ny = vel_index.shape
    nx = row_count * lat_count
    total_tiles = (nx // TB) * (ny // TB)
    tiles = total_tiles // devices
    slots = tiles * CAP
    trace_count = spectra.shape[2]
    data_rows = 2 * spectra.shape[1]
    features = data_rows + 3

    tile_id = tile_route[:, 0]
    order = jnp.arange(trace_count)
    rank = jnp.sum(
        ((tile_id[:, None] == tile_id[None, :]) & (order[:, None] < order[None, :])).astype(
            jnp.int32
        ),
        0,
    )
    slab_tiles = total_tiles // lat_count
    owner = (tile_id % slab_tiles) // tiles * lat_count + tile_id // slab_tiles
    slot = owner * slots + (tile_id % tiles) * CAP + rank
    cell_x = (bin_in_tile // TB).astype(jnp.float32) + trace_offset[0]
    cell_y = (bin_in_tile % TB).astype(jnp.float32) + trace_offset[1]
    padded_rows = -(-features // 16) * 16
    feats = jnp.concatenate(
        [
            spectra.reshape(data_rows, trace_count),
            weights[None],
            jnp.cos(math.pi * (cell_x[None] + 0.5) / TB),
            jnp.cos(math.pi * (cell_y[None] + 0.5) / TB),
            jnp.zeros((padded_rows - features, trace_count), jnp.float32),
        ],
        0,
    )
    placed = call(
        route_kernel, shaped(padded_rows, devices * slots), 1 << 28, slot[None], feats
    )
    sent = placed[:features].reshape(features, devices, slots).transpose(1, 0, 2)
    got = lax.all_to_all(sent, ("freq", "lat"), split_axis=0, concat_axis=0, tiled=True)
    got = got.transpose(1, 0, 2).reshape(features, devices * slots)
    coeffs = call(
        functools.partial(fit_kernel, tiles),
        shaped(tiles, TERMS, data_rows),
        1 << 30,
        got,
        scratch=[pltpu.VMEM((tiles, TERMS, TERMS + data_rows), jnp.float32)],
    )
    coeffs = coeffs.reshape(tiles, TERMS, 2, freq_count, -1).transpose(3, 0, 1, 2, 4)
    coeffs = lax.all_to_all(coeffs, "freq", split_axis=0, concat_axis=0, tiled=True)
    tile_rows = row_count // TB
    coeffs = coeffs.reshape(tile_rows, ny // TB, MODES, MODES, 2).transpose(4, 0, 2, 1, 3)
    mode_rows = tile_rows * MODES
    coeffs = coeffs.reshape(2 * mode_rows, ny // TB * MODES)

    high, low = dft_tables(nx)
    table = mode_tables(nx)
    high, low = jnp.asarray(high), jnp.asarray(low)
    table_y, table_x = jnp.asarray(table), jnp.asarray(np.ascontiguousarray(table.T))
    band = ny // lat_count
    refs = 2
    per_group = slowness.shape[1] // refs
    lat_at = lax.axis_index("lat")
    ky_index = lat_at * band + jnp.arange(2 * band) % band
    ky_vals = 2.0 * math.pi / ny * jnp.where(ky_index >= ny // 2, ky_index - ny, ky_index).astype(
        jnp.float32
    )
    kx_index = jnp.arange(nx)
    kx_vals = 2.0 * math.pi / nx * jnp.where(kx_index >= nx // 2, kx_index - nx, kx_index).astype(
        jnp.float32
    )
    odd_sign = jnp.where(jnp.arange(2 * band) < band, -1.0, 1.0)
    inverse_scale = 1.0 / (nx * ny)

    packed = call(
        modes_y_kernel, shaped(lat_count, mode_rows, 2 * band), 1 << 26, coeffs, table_y
    )
    images = []
    for depth_at in range(steps):
        table_row = slowness[depth_at]
        references = table_row.reshape(refs, per_group).mean(axis=1)
        wave_num = frequency[0] * references
        vertical = (
            (wave_num * wave_num)[:, None, None]
            - (kx_vals * kx_vals)[None, :, None]
            - (ky_vals * ky_vals)[None, None, :]
        )
        phase = jnp.sqrt(jnp.maximum(vertical, 0.0)) * depth_step
        damped = jnp.exp(-jnp.sqrt(jnp.maximum(-vertical, 0.0)) * depth_step)
        even = damped * jnp.cos(phase)
        odd = damped * jnp.sin(phase) * odd_sign
        velocity = vel_index[depth_at]
        picked = velocity[None] == jnp.arange(slowness.shape[1])[:, None, None]
        shift_of = (table_row.reshape(refs, per_group) - references[:, None]).reshape(-1)
        split_phase = (
            frequency[0]
            * jnp.sum(jnp.where(picked, shift_of[:, None, None], 0.0), 0)
            * depth_step
        )
        group = velocity // per_group
        along = jnp.cos(split_phase) * inverse_scale
        across = jnp.sin(split_phase) * inverse_scale

        columns = lax.all_to_all(packed, "lat", split_axis=0, concat_axis=0, tiled=True)
        moved = call(
            functools.partial(column_kernel, depth_at == 0),
            shaped(lat_count, refs, row_count, 2 * band),
            1 << 30,
            high,
            low,
            table_x,
            columns,
            even,
            odd,
        )
        rows = lax.all_to_all(moved, "lat", split_axis=0, concat_axis=0, tiled=True)
        last = depth_at == steps - 1
        shapes = [shaped(2 if last else 1, row_count, ny)]
        if not last:
            shapes.append(shaped(lat_count, row_count, 2 * band))
        made = call(
            functools.partial(row_kernel, last),
            shapes,
            1 << 30,
            high,
            low,
            rows,
            along,
            across,
            group,
        )
        wave_field = made[0]
        if not last:
            packed = made[1]
        split = wave_field[0].reshape(row_count, freq_count, ny // freq_count).transpose(1, 0, 2)
        images.append(split)
    split = lax.all_to_all(jnp.stack(images, 1), "freq", split_axis=0, concat_axis=0, tiled=True)
    return (wave_field[:, None], jnp.sum(split, 0))


def solution(mesh):
    return jax.shard_map(
        local,
        mesh=mesh,
        in_specs=(
            P(None, None, ("freq", "lat")),
            P(("freq", "lat"), None),
            P(("freq", "lat")),
            P(None, ("freq", "lat")),
            P(("freq", "lat")),
            P("freq"),
            P(),
            P(None, "lat", None),
        ),
        out_specs=(P(None, "freq", "lat", None), P(None, "lat", "freq")),
        check_vma=False,
    )
```

```python
import functools
import math

import jax
import jax.numpy as jnp
import numpy as np
from jax import lax
from jax.experimental import pallas as pl
from jax.experimental.pallas import tpu as pltpu
from jax.sharding import PartitionSpec as P

TB = 32
MODES = 8
CAP = 8
TERMS = MODES * MODES

damping = 1.0
depth_step = 1.0

NN = (((1,), (0,)), ((), ()))
NT = (((1,), (1,)), ((), ()))
VMEM = pl.BlockSpec(memory_space=pltpu.VMEM)


def dft_tables(length):
    at = np.arange(length)
    angle = 2.0 * math.pi / length * (at[:, None] * at[None, :] % length)
    exact = np.stack([np.cos(angle), np.sin(angle)], 0)
    high = exact.astype(jnp.bfloat16)
    low = (exact - high.astype(np.float64)).astype(jnp.bfloat16)
    return high, low


def mode_tables(length):
    at = np.arange(length)
    angle = 2.0 * math.pi / length * (at[:, None] * at[None, :] % length)
    cosines = np.cos(math.pi * np.arange(MODES)[:, None] * (np.arange(TB)[None, :] + 0.5) / TB)
    fold = np.zeros((length // TB, MODES, length))
    for tile in range(length // TB):
        fold[tile, :, tile * TB : (tile + 1) * TB] = cosines
    fold = fold.reshape(length // TB * MODES, length)
    return np.concatenate([fold @ np.cos(angle), -(fold @ np.sin(angle))], 1).astype(np.float32)


def split2(x):
    high = x.astype(jnp.bfloat16)
    return high, (x - high.astype(jnp.float32)).astype(jnp.bfloat16)


def dot3(a, b, dims=NN):
    one = functools.partial(lax.dot_general, dimension_numbers=dims, preferred_element_type=jnp.float32)
    return one(a[0], b[0]) + (one(a[0], b[1]) + one(a[1], b[0]))


def route_kernel(slot_ref, feat_ref, out_ref):
    feats = feat_ref[...]
    high = feats.astype(jnp.bfloat16)
    rest = feats - high.astype(jnp.float32)
    middle = rest.astype(jnp.bfloat16)
    low = (rest - middle.astype(jnp.float32)).astype(jnp.bfloat16)
    parts = jnp.concatenate([high, middle, low], 0)
    rows = feats.shape[0]
    slot = slot_ref[...]
    width = 256
    for at in range(0, out_ref.shape[1], width):
        places = lax.broadcasted_iota(jnp.int32, (width, slot.shape[1]), 0) + at
        chosen = jnp.where(places == slot, 1.0, 0.0).astype(jnp.bfloat16)
        got = lax.dot_general(parts, chosen, NT, preferred_element_type=jnp.float32)
        out_ref[:, at : at + width] = got[:rows] + got[rows : 2 * rows] + got[2 * rows :]


def fit_kernel(tiles, got_ref, out_ref, system):
    count = got_ref.shape[1]
    data_rows = got_ref.shape[0] - 3
    weight = got_ref[data_rows : data_rows + 1, :]

    def chebyshev(cosine):
        terms = [jnp.ones_like(cosine), cosine]
        for _ in range(MODES - 2):
            terms.append(2.0 * cosine * terms[-1] - terms[-2])
        return terms

    along_x = chebyshev(got_ref[data_rows + 1 : data_rows + 2, :])
    along_y = jnp.concatenate(chebyshev(got_ref[data_rows + 2 : data_rows + 3, :]), 0)
    basis = jnp.concatenate([term * along_y for term in along_x], 0)
    right = jnp.concatenate([basis, got_ref[:data_rows, :]], 0)
    weighted = basis * weight
    lane = lax.broadcasted_iota(jnp.int32, (1, count), 1)
    tile_of = lax.div(lax.rem(lane, tiles * CAP), CAP)
    width = TERMS + data_rows
    eye = jnp.where(
        lax.broadcasted_iota(jnp.int32, (TERMS, width), 0)
        == lax.broadcasted_iota(jnp.int32, (TERMS, width), 1),
        damping,
        0.0,
    )
    left = jnp.concatenate([jnp.where(tile_of == tile, weighted, 0.0) for tile in range(tiles)], 0)
    summed = lax.dot_general(
        left, right, NT, preferred_element_type=jnp.float32, precision=lax.Precision.HIGHEST
    )
    system[...] = summed.reshape(tiles, TERMS, width) + eye[None]
    for k in range(TERMS):
        row = system[:, k : k + 1, :]
        scaled = row * (1.0 / row[:, :, k : k + 1])
        whole = system[...]
        system[...] = whole - whole[:, :, k : k + 1] * scaled
        system[:, k : k + 1, :] = scaled
    out_ref[...] = system[:, :, TERMS:]


def bands(real, imag, out_ref):
    count = out_ref.shape[0]
    band = real.shape[1] // count
    for dst in range(count):
        part = slice(dst * band, (dst + 1) * band)
        out_ref[dst] = jnp.concatenate([real[:, part], imag[:, part]], 1)


def modes_y_kernel(coef_ref, table_ref, out_ref):
    rows = coef_ref.shape[0] // 2
    length = table_ref.shape[1] // 2
    made = lax.dot_general(
        coef_ref[...],
        table_ref[...],
        NN,
        preferred_element_type=jnp.float32,
        precision=lax.Precision.HIGHEST,
    )
    real = made[:rows, :length] - made[rows:, length:]
    imag = made[:rows, length:] + made[rows:, :length]
    bands(real, imag, out_ref)


def swapped(x):
    half = x.shape[1] // 2
    return jnp.concatenate([x[:, half:], x[:, :half]], 1)


def column_kernel(from_modes, high_ref, low_ref, table_ref, got_ref, even_ref, odd_ref, out_ref):
    lanes = got_ref.shape[2]
    got = got_ref[...].reshape(-1, lanes)
    sign = jnp.where(lax.broadcasted_iota(jnp.int32, (1, lanes), 1) < lanes // 2, -1.0, 1.0)
    cosine = (high_ref[0], low_ref[0])
    sine = (high_ref[1], low_ref[1])
    if from_modes:
        length = table_ref.shape[0] // 2
        both = lax.dot_general(
            table_ref[...],
            got,
            NN,
            preferred_element_type=jnp.float32,
            precision=lax.Precision.HIGHEST,
        )
        spectrum = both[:length] + sign * swapped(both[length:])
    else:
        parts = split2(got)
        spectrum = dot3(cosine, parts) - sign * swapped(dot3(sine, parts))
    turned = swapped(spectrum)
    refs = even_ref.shape[0]
    moved = jnp.concatenate(
        [spectrum * even_ref[g] + turned * odd_ref[g] for g in range(refs)], 1
    )
    parts = split2(moved)
    straight = dot3(cosine, parts)
    crossed = dot3(sine, parts)
    rows = out_ref.shape[2]
    for g in range(refs):
        part = slice(g * lanes, (g + 1) * lanes)
        back = straight[:, part] + sign * swapped(crossed[:, part])
        for dst in range(out_ref.shape[0]):
            out_ref[dst, g] = back[dst * rows : (dst + 1) * rows]


def row_kernel(last, high_ref, low_ref, got_ref, cos_ref, sin_ref, group_ref, *out_refs):
    wave_ref = out_refs[0]
    count, refs, rows, lanes = got_ref.shape
    half = lanes // 2
    cosine = (high_ref[0], low_ref[0])
    sine = (high_ref[1], low_ref[1])
    real = jnp.concatenate(
        [got_ref[src, :, :, :half].reshape(refs * rows, half) for src in range(count)], 1
    )
    imag = jnp.concatenate(
        [got_ref[src, :, :, half:].reshape(refs * rows, half) for src in range(count)], 1
    )
    parts = split2(jnp.concatenate([real, imag], 0))
    straight = dot3(parts, cosine)
    crossed = dot3(parts, sine)
    total = refs * rows
    real = straight[:total] - crossed[total:]
    imag = straight[total:] + crossed[:total]
    group = group_ref[...]
    chosen_real, chosen_imag = real[:rows], imag[:rows]
    for g in range(1, refs):
        part = slice(g * rows, (g + 1) * rows)
        chosen_real = jnp.where(group == g, real[part], chosen_real)
        chosen_imag = jnp.where(group == g, imag[part], chosen_imag)
    along, across = cos_ref[...], sin_ref[...]
    real = chosen_real * along - chosen_imag * across
    imag = chosen_real * across + chosen_imag * along
    wave_ref[0] = real
    if last:
        wave_ref[1] = imag
        return
    parts = split2(jnp.concatenate([real, imag], 0))
    straight = dot3(parts, cosine)
    crossed = dot3(parts, sine)
    bands(
        straight[:rows] + crossed[rows:],
        straight[rows:] - crossed[:rows],
        out_refs[1],
    )


def call(kernel, shapes, flops, *operands, scratch=()):
    single = not isinstance(shapes, (list, tuple))
    out_shape = jax.tree.map(
        lambda s: jax.ShapeDtypeStruct(s.shape, jnp.float32), shapes
    )
    return pl.pallas_call(
        kernel,
        out_shape=out_shape,
        in_specs=[VMEM] * len(operands),
        out_specs=VMEM if single else [VMEM] * len(shapes),
        scratch_shapes=list(scratch),
        cost_estimate=pl.CostEstimate(flops=flops, bytes_accessed=4 << 20, transcendentals=0),
        compiler_params=pltpu.CompilerParams(vmem_limit_bytes=48 << 20),
    )(*operands)


def exchange_kernel(count, in_ref, out_ref, sent, landed, kept):
    me = lax.axis_index("lat")
    barrier = pltpu.get_barrier_semaphore()
    partners = [lax.rem(me + step, count) for step in range(1, count)]
    for partner in partners:
        pl.semaphore_signal(
            barrier, inc=1, device_id={"lat": partner}, device_id_type=pl.DeviceIdType.MESH
        )
    pl.semaphore_wait(barrier, count - 1)
    copies = [
        pltpu.make_async_remote_copy(
            src_ref=in_ref.at[partner],
            dst_ref=out_ref.at[me],
            send_sem=sent.at[at],
            recv_sem=landed.at[at],
            device_id={"lat": partner},
            device_id_type=pl.DeviceIdType.MESH,
        )
        for at, partner in enumerate(partners)
    ]
    for copy in copies:
        copy.start()
    own = pltpu.make_async_copy(in_ref.at[me], out_ref.at[me], kept)
    own.start()
    own.wait()
    for copy in copies:
        copy.wait()


def exchange(blocks, number):
    count = blocks.shape[0]
    return pl.pallas_call(
        functools.partial(exchange_kernel, count),
        out_shape=jax.ShapeDtypeStruct(blocks.shape, blocks.dtype),
        in_specs=[pl.BlockSpec(memory_space=pl.ANY)],
        out_specs=pl.BlockSpec(memory_space=pl.ANY),
        scratch_shapes=[
            pltpu.SemaphoreType.DMA((count - 1,)),
            pltpu.SemaphoreType.DMA((count - 1,)),
            pltpu.SemaphoreType.DMA,
        ],
        compiler_params=pltpu.CompilerParams(
            collective_id=number, has_side_effects=True, vmem_limit_bytes=1 << 20
        ),
    )(blocks)


def shaped(*dims):
    return jax.ShapeDtypeStruct(dims, jnp.float32)


def local(spectra, tile_route, bin_in_tile, trace_offset, weights, frequency, slowness, vel_index):
    freq_count = lax.axis_size("freq")
    lat_count = lax.axis_size("lat")
    devices = freq_count * lat_count
    steps, row_count, ny = vel_index.shape
    nx = row_count * lat_count
    total_tiles = (nx // TB) * (ny // TB)
    tiles = total_tiles // devices
    slots = tiles * CAP
    trace_count = spectra.shape[2]
    data_rows = 2 * spectra.shape[1]
    features = data_rows + 3

    tile_id = tile_route[:, 0]
    order = jnp.arange(trace_count)
    rank = jnp.sum(
        ((tile_id[:, None] == tile_id[None, :]) & (order[:, None] < order[None, :])).astype(
            jnp.int32
        ),
        0,
    )
    slab_tiles = total_tiles // lat_count
    owner = (tile_id % slab_tiles) // tiles * lat_count + tile_id // slab_tiles
    slot = owner * slots + (tile_id % tiles) * CAP + rank
    cell_x = (bin_in_tile // TB).astype(jnp.float32) + trace_offset[0]
    cell_y = (bin_in_tile % TB).astype(jnp.float32) + trace_offset[1]
    padded_rows = -(-features // 16) * 16
    feats = jnp.concatenate(
        [
            spectra.reshape(data_rows, trace_count),
            weights[None],
            jnp.cos(math.pi * (cell_x[None] + 0.5) / TB),
            jnp.cos(math.pi * (cell_y[None] + 0.5) / TB),
            jnp.zeros((padded_rows - features, trace_count), jnp.float32),
        ],
        0,
    )
    placed = call(
        route_kernel, shaped(padded_rows, devices * slots), 1 << 28, slot[None], feats
    )
    sent = placed[:features].reshape(features, devices, slots).transpose(1, 0, 2)
    got = lax.all_to_all(sent, ("freq", "lat"), split_axis=0, concat_axis=0, tiled=True)
    got = got.transpose(1, 0, 2).reshape(features, devices * slots)
    coeffs = call(
        functools.partial(fit_kernel, tiles),
        shaped(tiles, TERMS, data_rows),
        1 << 30,
        got,
        scratch=[pltpu.VMEM((tiles, TERMS, TERMS + data_rows), jnp.float32)],
    )
    coeffs = coeffs.reshape(tiles, TERMS, 2, freq_count, -1).transpose(3, 0, 1, 2, 4)
    coeffs = lax.all_to_all(coeffs, "freq", split_axis=0, concat_axis=0, tiled=True)
    tile_rows = row_count // TB
    coeffs = coeffs.reshape(tile_rows, ny // TB, MODES, MODES, 2).transpose(4, 0, 2, 1, 3)
    mode_rows = tile_rows * MODES
    coeffs = coeffs.reshape(2 * mode_rows, ny // TB * MODES)

    high, low = dft_tables(nx)
    table = mode_tables(nx)
    high, low = jnp.asarray(high), jnp.asarray(low)
    table_y, table_x = jnp.asarray(table), jnp.asarray(np.ascontiguousarray(table.T))
    band = ny // lat_count
    refs = 2
    per_group = slowness.shape[1] // refs
    lat_at = lax.axis_index("lat")
    ky_index = lat_at * band + jnp.arange(2 * band) % band
    ky_vals = 2.0 * math.pi / ny * jnp.where(ky_index >= ny // 2, ky_index - ny, ky_index).astype(
        jnp.float32
    )
    kx_index = jnp.arange(nx)
    kx_vals = 2.0 * math.pi / nx * jnp.where(kx_index >= nx // 2, kx_index - nx, kx_index).astype(
        jnp.float32
    )
    odd_sign = jnp.where(jnp.arange(2 * band) < band, -1.0, 1.0)
    inverse_scale = 1.0 / (nx * ny)

    packed = call(
        modes_y_kernel, shaped(lat_count, mode_rows, 2 * band), 1 << 26, coeffs, table_y
    )
    images = []
    for depth_at in range(steps):
        table_row = slowness[depth_at]
        references = table_row.reshape(refs, per_group).mean(axis=1)
        wave_num = frequency[0] * references
        vertical = (
            (wave_num * wave_num)[:, None, None]
            - (kx_vals * kx_vals)[None, :, None]
            - (ky_vals * ky_vals)[None, None, :]
        )
        phase = jnp.sqrt(jnp.maximum(vertical, 0.0)) * depth_step
        damped = jnp.exp(-jnp.sqrt(jnp.maximum(-vertical, 0.0)) * depth_step)
        even = damped * jnp.cos(phase)
        odd = damped * jnp.sin(phase) * odd_sign
        velocity = vel_index[depth_at]
        picked = velocity[None] == jnp.arange(slowness.shape[1])[:, None, None]
        shift_of = (table_row.reshape(refs, per_group) - references[:, None]).reshape(-1)
        split_phase = (
            frequency[0]
            * jnp.sum(jnp.where(picked, shift_of[:, None, None], 0.0), 0)
            * depth_step
        )
        group = velocity // per_group
        along = jnp.cos(split_phase) * inverse_scale
        across = jnp.sin(split_phase) * inverse_scale

        if depth_at == 0:
            columns = lax.all_to_all(packed, "lat", split_axis=0, concat_axis=0, tiled=True)
        else:
            columns = exchange(packed, 2 * depth_at)
        moved = call(
            functools.partial(column_kernel, depth_at == 0),
            shaped(lat_count, refs, row_count, 2 * band),
            1 << 30,
            high,
            low,
            table_x,
            columns,
            even,
            odd,
        )
        rows = exchange(moved, 2 * depth_at + 1)
        last = depth_at == steps - 1
        shapes = [shaped(2 if last else 1, row_count, ny)]
        if not last:
            shapes.append(shaped(lat_count, row_count, 2 * band))
        made = call(
            functools.partial(row_kernel, last),
            shapes,
            1 << 30,
            high,
            low,
            rows,
            along,
            across,
            group,
        )
        wave_field = made[0]
        if not last:
            packed = made[1]
        split = wave_field[0].reshape(row_count, freq_count, ny // freq_count).transpose(1, 0, 2)
        images.append(split)
    split = lax.all_to_all(jnp.stack(images, 1), "freq", split_axis=0, concat_axis=0, tiled=True)
    return (wave_field[:, None], jnp.sum(split, 0))


def solution(mesh):
    return jax.shard_map(
        local,
        mesh=mesh,
        in_specs=(
            P(None, None, ("freq", "lat")),
            P(("freq", "lat"), None),
            P(("freq", "lat")),
            P(None, ("freq", "lat")),
            P(("freq", "lat")),
            P("freq"),
            P(),
            P(None, "lat", None),
        ),
        out_specs=(P(None, "freq", "lat", None), P(None, "lat", "freq")),
        check_vma=False,
    )
```
